8 devices in a mesh: dp: 2 (over z, y), dap: 4 (over x, core).
Axes of the slice: x: 2, y: 2, z: 1, core: 2. Of those that a mesh axis runs over, the one named last changes fastest.
Arguments:
- pair_act: bfloat16 [2, 1024, 1024, 128], P('dp', 'dap')
- pair_mask: int32 [2, 1024, 1024], P('dp', 'dap')
- true_bin: int32 [2, 1024, 1024], P('dp', 'dap')
- msa_act: bfloat16 [2, 16, 1024, 256], P('dp', None, 'dap')
- msa_true: int32 [2, 16, 1024], P('dp', None, 'dap')
- bert_mask: int32 [2, 16, 1024], P('dp', None, 'dap')
- w_dist: bfloat16 [128, 64], replicated
- b_dist: float32 [64], replicated
- w_msa: bfloat16 [256, 23], replicated
- b_msa: float32 [23], replicated
Outputs:
- output 1: float32 [], replicated
- output 2: bfloat16 [2, 1024, 1024, 128], P('dp', 'dap')
- output 3: bfloat16 [2, 16, 1024, 256], P('dp', None, 'dap')
- output 4: float32 [128, 64], replicated
- output 5: float32 [64], replicated
- output 6: float32 [256, 23], replicated
- output 7: float32 [23], replicated
All inputs are finite; a program needn't handle non-finite values.
Results may differ from the reference program's by a relative error of at most 0.00790914.
Values are sent between devices in bfloat16 or wider.
A program may use at most 1 GiB of HBM per device.

```python
import math
import jax
import jax.numpy as jnp
from jax import lax

BATCH = 2
RES = 1024
SEQS = 16
C_Z = 128
C_M = 256
BINS = 64
CLASSES = 23
ROW_BLOCK = math.gcd(RES, 32)
ROW_STEPS = RES // ROW_BLOCK
LOSS_SCALE = 2.0 ** 16
DIST_WEIGHT = 0.3
MSA_WEIGHT = 2.0
DIST_EPS = 1e-6
MSA_EPS = 1e-8


def setup_inputs(seed: int = 0) -> dict:
    rng_keys = jax.random.split(jax.random.key(seed), 13)
    act_scale = jax.random.uniform(rng_keys[0], (BATCH, 1, 1, 1), minval=0.5, maxval=2.0)
    pair_act = (jax.random.normal(rng_keys[1], (BATCH, RES, RES, C_Z)) * act_scale).astype(jnp.bfloat16)
    lengths = jax.random.randint(rng_keys[2], (BATCH, 1), RES // 2, RES + 1)
    positions = jnp.arange(RES)[None, :]
    present = (jax.random.randint(rng_keys[3], (BATCH, RES), 0, 10) > 0) & (positions < lengths)
    pair_mask = (present[:, :, None] & present[:, None, :]).astype(jnp.int32)
    true_bin = jax.random.randint(rng_keys[4], (BATCH, RES, RES), 0, BINS)
    msa_act = jax.random.normal(rng_keys[5], (BATCH, SEQS, RES, C_M)).astype(jnp.bfloat16)
    msa_true = jax.random.randint(rng_keys[6], (BATCH, SEQS, RES), 0, CLASSES)
    block_rate = jax.random.randint(rng_keys[7], (BATCH, 1, RES // 8), 0, 31)
    mask_rate = jnp.repeat(block_rate, 8, axis=2)
    mask_draw = jax.random.randint(rng_keys[8], (BATCH, SEQS, RES), 0, 100)
    bert_mask = ((mask_draw < mask_rate) & (positions < lengths)[:, None, :]).astype(jnp.int32)
    w_dist = (jax.random.normal(rng_keys[9], (C_Z, BINS)) * (1.5 * C_Z ** -0.5)).astype(jnp.bfloat16)
    b_dist = jax.random.normal(rng_keys[10], (BINS,))
    w_msa = (jax.random.normal(rng_keys[11], (C_M, CLASSES)) * (1.5 * C_M ** -0.5)).astype(jnp.bfloat16)
    b_msa = jax.random.normal(rng_keys[12], (CLASSES,))
    return {'pair_act': pair_act, 'pair_mask': pair_mask, 'true_bin': true_bin, 'msa_act': msa_act,
            'msa_true': msa_true, 'bert_mask': bert_mask, 'w_dist': w_dist, 'b_dist': b_dist,
            'w_msa': w_msa, 'b_msa': b_msa}


def class_terms(logits, labels):
    log_prob = jax.nn.log_softmax(logits, axis=-1)
    onehot = jax.nn.one_hot(labels, logits.shape[-1], dtype=jnp.float32)
    return -jnp.sum(log_prob * onehot, axis=-1), jnp.exp(log_prob) - onehot


def reference(pair_act, pair_mask, true_bin, msa_act, msa_true, bert_mask, w_dist, b_dist, w_msa, b_msa):
    starts = jnp.arange(ROW_STEPS) * ROW_BLOCK

    def protein_terms(operands):
        pair_one, mask_one, bin_one, msa_one, true_one, bert_one = operands
        mask_f = mask_one.astype(jnp.float32)
        pair_den = DIST_EPS + jnp.sum(mask_f)
        msa_den = MSA_EPS + jnp.sum(bert_one.astype(jnp.float32))
        dist_scale = LOSS_SCALE * DIST_WEIGHT / BATCH / pair_den
        msa_scale = LOSS_SCALE * MSA_WEIGHT / BATCH / msa_den

        def dist_rows(row_start):
            pair_rows = lax.dynamic_slice_in_dim(pair_one, row_start, ROW_BLOCK, axis=0)
            pair_cols = lax.dynamic_slice_in_dim(pair_one, row_start, ROW_BLOCK, axis=1)
            mask_rows = lax.dynamic_slice_in_dim(mask_f, row_start, ROW_BLOCK, axis=0)
            bin_rows = lax.dynamic_slice_in_dim(bin_one, row_start, ROW_BLOCK, axis=0)
            direct = jnp.dot(pair_rows.reshape(-1, C_Z), w_dist, preferred_element_type=jnp.float32)
            mirror = jnp.dot(pair_cols.reshape(-1, C_Z), w_dist, preferred_element_type=jnp.float32)
            logits = (direct.reshape(ROW_BLOCK, RES, BINS)
                      + jnp.swapaxes(mirror.reshape(RES, ROW_BLOCK, BINS), 0, 1) + b_dist)
            neg_logp, prob_diff = class_terms(logits, bin_rows)
            grad_rows = (prob_diff * (mask_rows * dist_scale)[:, :, None]).astype(jnp.bfloat16)
            return jnp.sum(neg_logp * mask_rows), grad_rows

        dist_sums, grad_blocks = lax.map(dist_rows, starts)
        grad_pair = grad_blocks.reshape(RES, RES, BINS)

        def back_rows(row_start):
            pair_rows = lax.dynamic_slice_in_dim(pair_one, row_start, ROW_BLOCK, axis=0)
            pair_cols = lax.dynamic_slice_in_dim(pair_one, row_start, ROW_BLOCK, axis=1)
            g_rows = lax.dynamic_slice_in_dim(grad_pair, row_start, ROW_BLOCK, axis=0)
            g_cols = lax.dynamic_slice_in_dim(grad_pair, row_start, ROW_BLOCK, axis=1)
            direct = jnp.dot(g_rows.reshape(-1, BINS), w_dist.T, preferred_element_type=jnp.float32)
            mirror = jnp.dot(g_cols.reshape(-1, BINS), w_dist.T, preferred_element_type=jnp.float32)
            grad_rows = (direct.reshape(ROW_BLOCK, RES, C_Z)
                         + jnp.swapaxes(mirror.reshape(RES, ROW_BLOCK, C_Z), 0, 1)).astype(jnp.bfloat16)
            g_swap = jnp.swapaxes(g_rows, 0, 1).reshape(-1, BINS)
            w_part = (jnp.dot(pair_rows.reshape(-1, C_Z).T, g_rows.reshape(-1, BINS), preferred_element_type=jnp.float32)
                      + jnp.dot(pair_cols.reshape(-1, C_Z).T, g_swap, preferred_element_type=jnp.float32))
            return grad_rows, w_part

        grad_z_blocks, w_blocks = lax.map(back_rows, starts)
        grad_z = grad_z_blocks.reshape(RES, RES, C_Z)

        def msa_rows(row_operands):
            act_row, true_row, bert_row = row_operands
            logits = jnp.dot(act_row, w_msa, preferred_element_type=jnp.float32) + b_msa
            neg_logp, prob_diff = class_terms(logits, true_row)
            bert_f = bert_row.astype(jnp.float32)
            grad_row = (prob_diff * (bert_f * msa_scale)[:, None]).astype(jnp.bfloat16)
            grad_act = jnp.dot(grad_row, w_msa.T, preferred_element_type=jnp.float32).astype(jnp.bfloat16)
            w_part = jnp.dot(act_row.T, grad_row, preferred_element_type=jnp.float32)
            return jnp.sum(neg_logp * bert_f), grad_act, w_part, jnp.sum(grad_row.astype(jnp.float32), axis=0)

        msa_sums, grad_m, msa_w_parts, msa_b_parts = lax.map(msa_rows, (msa_one, true_one, bert_one))
        loss_one = DIST_WEIGHT * jnp.sum(dist_sums) / pair_den + MSA_WEIGHT * jnp.sum(msa_sums) / msa_den
        return (loss_one, grad_z, grad_m, jnp.sum(w_blocks, axis=0),
                jnp.sum(grad_pair.astype(jnp.float32), axis=(0, 1)),
                jnp.sum(msa_w_parts, axis=0), jnp.sum(msa_b_parts, axis=0))

    losses, grad_z, grad_m, dist_w, dist_b, msa_w, msa_b = lax.map(
        protein_terms, (pair_act, pair_mask, true_bin, msa_act, msa_true, bert_mask))
    return (jnp.mean(losses), grad_z, grad_m, jnp.sum(dist_w, axis=0), jnp.sum(dist_b, axis=0),
            jnp.sum(msa_w, axis=0), jnp.sum(msa_b, axis=0))
```

```python
import functools

import jax
import jax.numpy as jnp
from jax import lax
from jax.experimental import pallas as pl
from jax.experimental.pallas import tpu as pltpu
from jax.sharding import PartitionSpec as P

LOSS_SCALE = 2.0 ** 16
DIST_WEIGHT = 0.3
MSA_WEIGHT = 2.0
DIST_EPS = 1e-6
MSA_EPS = 1e-8
BINS = 64
CZ = 128
TI = 16
TJ = 128
KS = 72
F32 = jnp.float32
BF16 = jnp.bfloat16


def dot(a, b, dims=((1,), (0,))):
    return lax.dot_general(a, b, (dims, ((), ())), preferred_element_type=F32)


def grads(oa, ob, ea, eb, umat, vmat_a, vmat_b):
    ga = jnp.where(ea >= 0, jnp.where(oa, vmat_a, umat), 0.0)
    gb = jnp.where(eb >= 0, jnp.where(ob, vmat_b, umat), 0.0)
    return ga, gb


def pair_kernel(both, chained, idx_ref, scale_ref, za_ref, zb_ref, ea_ref, eb_ref, wbd_ref, wdup_ref, b2_ref, w2t_ref, *refs):
    if chained:
        refs = refs[1:]
    if both:
        dz_ref, dw_ref, db_ref, loss_ref, u_ref, d2_ref, v_ref = refs
    else:
        dz_ref, dw_ref, db_ref, loss_ref, d2_ref = refs
    step = pl.program_id(1)

    @pl.when((pl.program_id(0) == 0) & (step == 0))
    def _():
        dw_ref[...] = jnp.zeros_like(dw_ref)
        db_ref[...] = jnp.zeros_like(db_ref)
        loss_ref[...] = jnp.zeros_like(loss_ref)

    scale = scale_ref[0]
    d2_ref[...] = dot(zb_ref[...].reshape(TJ * TI, CZ), wdup_ref[...])
    kio = lax.broadcasted_iota(jnp.int32, (BINS, TJ), 0)
    low = lax.broadcasted_iota(jnp.int32, (TJ, 2 * BINS), 1) < BINS

    def two_rows(q, carry):
        i0 = 2 * q
        z0, z1 = za_ref[i0], za_ref[i0 + 1]
        mirror = jnp.where(low, d2_ref[pl.ds(i0, TJ, stride=TI), :], d2_ref[pl.ds(i0 + 1, TJ, stride=TI), :])
        logits = dot(jnp.concatenate([z0, z1], axis=1), wbd_ref[...]) + mirror + b2_ref[...]
        logits_t = logits.T
        gts = []
        for h in range(2):
            i = i0 + h
            lg = logits_t[h * BINS:(h + 1) * BINS]
            top = jnp.max(lg, axis=0, keepdims=True)
            ex = jnp.exp(lg - top)
            tot = jnp.sum(ex, axis=0, keepdims=True)
            p = ex * (1.0 / tot)
            lse = top + jnp.log(tot)
            ea = ea_ref[pl.ds(i, 1), :]
            eb = eb_ref[pl.ds(i, 1), :]
            oa = kio == ea
            ob = kio == eb
            um = p * scale
            vm = (p - 1.0) * scale
            ga, gb = grads(oa, ob, ea, eb, um, vm, vm)
            nll = jnp.where(ea >= 0, lse, 0.0)
            hit = jnp.where(oa, lg, 0.0)
            if both:
                nll = nll + jnp.where(eb >= 0, lse, 0.0)
                hit = hit + jnp.where(ob, lg, 0.0)
            loss_ref[...] += nll - jnp.sum(hit, axis=0, keepdims=True)
            ga, gb = ga.astype(BF16), gb.astype(BF16)
            db_ref[...] += ga.astype(F32)
            if both:
                db_ref[...] += gb.astype(F32)
                row = step * TI + i
                u_ref[row] = um.astype(BF16)
                v_ref[pl.ds(row, 1), :] = jnp.sum(jnp.where(oa, vm, 0.0), axis=0, keepdims=True)
                v_ref[pl.ds(128 + row, 1), :] = jnp.sum(jnp.where(ob, vm, 0.0), axis=0, keepdims=True)
            gt = jnp.concatenate([ga, gb], axis=0)
            dz_ref[i] = dot(gt, w2t_ref[...], ((0,), (0,))).astype(BF16)
            gts.append(gt)
        dw_ref[...] += dot(jnp.concatenate(gts, axis=1), jnp.concatenate([z0, z1], axis=0))
        return carry

    lax.fori_loop(0, TI // 2, two_rows, 0, unroll=2)
    if both:
        @pl.when(step == pl.num_programs(1) - 1)
        def _():
            u_ref[128:132] = v_ref[...].astype(BF16).reshape(4, BINS, TJ)


def back_kernel(idx_ref, za_ref, u_ref, ea_ref, eb_ref, w2t_ref, prev_ref, dz_ref, dw_ref, s_ref, t_ref, v_ref):
    step = pl.program_id(0)

    @pl.when(step == 0)
    def _():
        dw_ref[...] = jnp.zeros_like(dw_ref)

        def widen(j, carry):
            s_ref[pl.ds(pl.multiple_of(j * KS, 8), BINS), :] = u_ref[j].astype(F32)
            return carry

        lax.fori_loop(0, TJ, widen, 0, unroll=4)

        def swap(k, carry):
            t_ref[pl.ds(k, TJ, stride=KS), :] = s_ref[pl.ds(k, TJ, stride=KS), :].T
            return carry

        lax.fori_loop(0, BINS, swap, 0, unroll=2)
        vals = u_ref[128:132].astype(F32).reshape(2, TJ, TJ)
        v_ref[0:TJ] = vals[1].T
        v_ref[TJ:2 * TJ] = vals[0].T

    kio = lax.broadcasted_iota(jnp.int32, (BINS, TJ), 0)

    def two_rows(q, carry):
        gts = []
        for h in range(2):
            i = 2 * q + h
            row = step * TI + i
            um = t_ref[pl.ds(pl.multiple_of(row * KS, 8), BINS), :]
            ea = ea_ref[pl.ds(i, 1), :]
            eb = eb_ref[pl.ds(i, 1), :]
            ga, gb = grads(kio == ea, kio == eb, ea, eb, um,
                           v_ref[pl.ds(row, 1), :], v_ref[pl.ds(TJ + row, 1), :])
            gt = jnp.concatenate([ga.astype(BF16), gb.astype(BF16)], axis=0)
            dz_ref[i] = dot(gt, w2t_ref[...], ((0,), (0,))).astype(BF16)
            gts.append(gt)
        zz = jnp.concatenate([za_ref[2 * q], za_ref[2 * q + 1]], axis=0)
        dw_ref[...] += dot(jnp.concatenate(gts, axis=1), zz)
        return carry

    lax.fori_loop(0, TI // 2, two_rows, 0, unroll=2)


def const_spec(shape):
    return pl.BlockSpec(shape, lambda *a: (0,) * len(shape))


def pair_call(name, idx, grid, maps, both, scale, z, zb, ea, eb, weights, dz_shape, dz_prev, cost):
    za_map, zb_map, ea_map, eb_map = maps
    in_specs = [
        pl.BlockSpec(memory_space=pltpu.SMEM),
        pl.BlockSpec((TI, TJ, CZ), za_map),
        pl.BlockSpec((TJ, TI, CZ), zb_map),
        pl.BlockSpec((TI, TJ), ea_map),
        pl.BlockSpec((TI, TJ), eb_map),
        const_spec((256, 128)), const_spec((128, 128)), const_spec((1, 128)), const_spec((128, 128)),
    ]
    args = [idx, scale, z, zb, ea, eb, *weights]
    aliases = {}
    if dz_prev is not None:
        in_specs.append(pl.BlockSpec(memory_space=pl.ANY))
        args.append(dz_prev)
        aliases = {len(args) - 1: 0}
    out_shape = [jax.ShapeDtypeStruct(dz_shape, BF16), jax.ShapeDtypeStruct((128, CZ), F32),
                 jax.ShapeDtypeStruct((BINS, TJ), F32), jax.ShapeDtypeStruct((1, TJ), F32)]
    out_specs = [pl.BlockSpec((TI, TJ, CZ), za_map), const_spec((128, CZ)), const_spec((BINS, TJ)), const_spec((1, TJ))]
    scratch = [pltpu.VMEM((TJ * TI, 128), F32)]
    if both:
        out_shape.append(jax.ShapeDtypeStruct((132, BINS, TJ), BF16))
        out_specs.append(const_spec((132, BINS, TJ)))
        scratch.append(pltpu.VMEM((256, TJ), F32))
    return pl.pallas_call(
        functools.partial(pair_kernel, both, dz_prev is not None),
        out_shape=out_shape,
        grid_spec=pltpu.PrefetchScalarGridSpec(num_scalar_prefetch=1, grid=grid, in_specs=in_specs,
                                               out_specs=out_specs, scratch_shapes=scratch),
        input_output_aliases=aliases,
        compiler_params=pltpu.CompilerParams(vmem_limit_bytes=40 * 2 ** 20),
        cost_estimate=pl.CostEstimate(flops=cost, bytes_accessed=16 * 2 ** 20, transcendentals=0),
        name=name,
    )(*args)


def back_call(name, idx, maps, z, u, ea, eb, w2t, dz_prev, cost):
    za_map, eb_map = maps[0], maps[2]
    return pl.pallas_call(
        back_kernel,
        out_shape=[jax.ShapeDtypeStruct(dz_prev.shape, BF16), jax.ShapeDtypeStruct((128, CZ), F32)],
        grid_spec=pltpu.PrefetchScalarGridSpec(
            num_scalar_prefetch=1, grid=(TJ // TI,),
            in_specs=[pl.BlockSpec((TI, TJ, CZ), za_map), const_spec((132, BINS, TJ)),
                      pl.BlockSpec((TI, TJ), maps[1]), pl.BlockSpec((TI, TJ), eb_map),
                      const_spec((128, 128)), pl.BlockSpec(memory_space=pl.ANY)],
            out_specs=[pl.BlockSpec((TI, TJ, CZ), za_map), const_spec((128, CZ))],
            scratch_shapes=[pltpu.VMEM((TJ * KS, TJ), F32), pltpu.VMEM((TJ * KS, TJ), F32),
                            pltpu.VMEM((2 * TJ, TJ), F32)]),
        input_output_aliases={6: 0},
        compiler_params=pltpu.CompilerParams(vmem_limit_bytes=40 * 2 ** 20),
        cost_estimate=pl.CostEstimate(flops=cost, bytes_accessed=16 * 2 ** 20, transcendentals=0),
        name=name,
    )(idx, z, u, ea, eb, w2t, dz_prev)


def class_terms(logits, labels):
    log_prob = jax.nn.log_softmax(logits, axis=-1)
    onehot = jax.nn.one_hot(labels, logits.shape[-1], dtype=F32)
    return -jnp.sum(log_prob * onehot, axis=-1), jnp.exp(log_prob) - onehot


def swap_with(x, mask):
    return lax.ppermute(x, 'dap', [(i, i ^ mask) for i in range(4)])


def solution(mesh):
    dp_size = mesh.shape['dp']
    pair_spec = P('dp', 'dap', None, None)
    pair_int_spec = P('dp', 'dap', None)
    msa_spec = P('dp', None, 'dap', None)
    msa_int_spec = P('dp', None, 'dap')

    def local_step(pair_act, pair_mask, true_bin, msa_act, msa_true, bert_mask, w_dist, b_dist, w_msa, b_msa):
        batch_total = pair_act.shape[0] * dp_size
        z, mask = pair_act[0], pair_mask[0]
        rows = z.shape[0]
        half = rows // 2
        me = lax.axis_index('dap').astype(jnp.int32)
        side = me // 2
        label = jnp.where(mask > 0, true_bin[0], -1)

        lab_of, z_of = {}, {}
        for other in (2, 3, 1):
            p = me ^ other
            lab_of[other] = swap_with(lax.dynamic_slice_in_dim(label, p * rows, rows, axis=1), other)
        p = me ^ 1
        z_of[1] = swap_with(lax.dynamic_slice(z, (0, p * rows, 0), (rows, rows, CZ)), 1)
        for n in range(2):
            for other in (2, 3):
                p = me ^ other
                far = jnp.bitwise_xor(side, 1 - n)
                part = lax.dynamic_slice(z, (n * half, p * rows + far * half, 0), (half, half, CZ))
                z_of[other, n] = swap_with(part, other)

        bert_f = bert_mask.astype(F32)
        counts = lax.psum(jnp.stack([jnp.sum(mask.astype(F32)), jnp.sum(bert_f)]), 'dap')
        pair_den = DIST_EPS + counts[0]
        msa_den = MSA_EPS + counts[1]
        dist_scale = LOSS_SCALE * DIST_WEIGHT / batch_total / pair_den
        msa_scale = LOSS_SCALE * MSA_WEIGHT / batch_total / msa_den

        zero = jnp.zeros((CZ, BINS), BF16)
        wbd = jnp.concatenate([jnp.concatenate([w_dist, zero], 1), jnp.concatenate([zero, w_dist], 1)], 0)
        wdup = jnp.concatenate([w_dist, w_dist], 1)
        b2 = jnp.concatenate([b_dist, b_dist])[None, :]
        w2t = jnp.concatenate([w_dist.T, w_dist.T], 0)
        weights = (wbd, wdup, b2, w2t)
        scale = dist_scale[None]
        per = rows // TI
        hper = half // TI
        lab_t = {k: v.T for k, v in lab_of.items()}
        lab_t[0] = lax.dynamic_slice_in_dim(label, me * rows, rows, axis=1).T

        idx0 = jnp.stack([me * (rows // TJ), me * per])
        dz, dw0, db0, ls0 = pair_call(
            'own', idx0, (rows // TJ, per),
            (lambda c, s, r: (s, r[0] + c, 0), lambda c, s, r: (c, r[1] + s, 0),
             lambda c, s, r: (s, r[0] + c), lambda c, s, r: (s, c)),
            False, scale, z, z, label, lab_t[0], weights, z.shape, None, 30_000_000)
        idx1 = jnp.stack([(me ^ 1) * (rows // TJ), me * per])
        dz, dw1, db1, ls1 = pair_call(
            'near', idx1, (rows // TJ, per),
            (lambda c, s, r: (s, r[0] + c, 0), lambda c, s, r: (c, s, 0),
             lambda c, s, r: (s, r[0] + c), lambda c, s, r: (s, c)),
            False, scale, z, z_of[1], label, lab_t[1], weights, z.shape, dz, 30_000_000)
        dws, dbs, losses, u_of = [dw0, dw1], [db0, db1], [ls0, ls1], {}
        for n in range(2):
            for other in (2, 3):
                idx = jnp.stack([jnp.bitwise_xor(side, n) * hper, (me ^ other) * (rows // TJ) + n])
                dz, dw, db, ls, u = pair_call(
                    'far', idx, (1, hper),
                    (lambda c, s, r: (r[0] + s, r[1], 0), lambda c, s, r: (0, s, 0),
                     lambda c, s, r: (r[0] + s, r[1]), lambda c, s, r, n=n: (r[0] + s, n)),
                    True, scale, z, z_of[other, n], label, lab_t[other], weights, z.shape, dz, 15_000_000)
                dws.append(dw), dbs.append(db), losses.append(ls)
                u_of[other, n] = swap_with(u, other)
        for n in range(2):
            for other in (2, 3):
                far = jnp.bitwise_xor(side, 1 - n)
                idx = jnp.stack([(me ^ other) * (rows // TJ) + far, far])
                dz, dw = back_call(
                    'back', idx,
                    (lambda s, r, n=n: (n * hper + s, r[0], 0), lambda s, r, n=n: (n * hper + s, r[0]),
                     lambda s, r, n=n: (n * hper + s, r[1])),
                    z, u_of[other, n], label, lab_t[other], w2t, dz, 8_000_000)
                dws.append(dw)

        msa_logits = jnp.einsum('bsrc,ck->bsrk', msa_act, w_msa, preferred_element_type=F32) + b_msa
        msa_nll, msa_diff = class_terms(msa_logits, msa_true)
        grad_h = (msa_diff * (bert_f * msa_scale)[..., None]).astype(BF16)
        grad_m = jnp.einsum('bsrk,ck->bsrc', grad_h, w_msa, preferred_element_type=F32).astype(BF16)
        dw_msa = jnp.einsum('bsrc,bsrk->ck', msa_act, grad_h, preferred_element_type=F32)
        db_msa = jnp.sum(grad_h, axis=(0, 1, 2), dtype=F32)

        dw = sum(dws)
        dw = (dw[:BINS] + dw[BINS:]).T
        db = jnp.sum(sum(dbs), axis=1)
        loss = (DIST_WEIGHT * jnp.sum(sum(losses)) / pair_den + MSA_WEIGHT * jnp.sum(msa_nll * bert_f) / msa_den)
        total, dw, db, dw_msa, db_msa = lax.psum((loss / batch_total, dw, db, dw_msa, db_msa), ('dp', 'dap'))
        return total, dz[None], grad_m, dw, db, dw_msa, db_msa

    return jax.shard_map(local_step, mesh=mesh,
                         in_specs=(pair_spec, pair_int_spec, pair_int_spec, msa_spec, msa_int_spec, msa_int_spec,
                                   P(), P(), P(), P()),
                         out_specs=(P(), pair_spec, msa_spec, P(), P(), P(), P()),
                         check_vma=False)
```
